32 devices in a mesh: dp: 4 (over z), seq: 4 (over y, core), tensor: 2 (over x).
Axes of the slice: x: 2, y: 2, z: 4, core: 2. Of those that a mesh axis runs over, the one named last changes fastest.
Arguments:
- tokens: bfloat16 [4, 512, 2048], P('dp', 'seq'), may hold values from -6 to 6
- positions: int32 [4, 512], P('dp', 'seq'), may hold values from 0 to 1533, as said below
- gain_attn: bfloat16 [1, 2048], P(None, ('dp', 'seq')), may hold values from 0.5 to 1.5
- gain_ffn: bfloat16 [1, 2048], P(None, ('dp', 'seq')), may hold values from 0.5 to 1.5
- w_query: bfloat16 [1, 2048, 2048], P(None, ('dp', 'seq'), 'tensor'), may hold values from -1 to 1
- w_key: bfloat16 [1, 2048, 512], P(None, ('dp', 'seq'), 'tensor'), may hold values from -1 to 1
- w_value: bfloat16 [1, 2048, 512], P(None, ('dp', 'seq'), 'tensor'), may hold values from -0.125 to 0.125
- w_out: bfloat16 [1, 2048, 2048], P(None, ('dp', 'seq'), 'tensor'), may hold values from -0.75 to 0.75
- w_gate: bfloat16 [1, 2048, 8192], P(None, ('dp', 'seq'), 'tensor'), may hold values from -0.125 to 0.125
- w_up: bfloat16 [1, 2048, 8192], P(None, ('dp', 'seq'), 'tensor'), may hold values from -0.125 to 0.125
- w_down: bfloat16 [1, 2048, 8192], P(None, ('dp', 'seq'), 'tensor'), may hold values from -0.0625 to 0.0625
- cotangent: bfloat16 [4, 512, 2048], P('dp', 'seq'), may hold values from -6 to 6
Outputs:
- activations: bfloat16 [4, 512, 2048], P('dp', 'seq')
- input_grad: float32 [4, 512, 2048], P('dp', 'seq')
- grad_gain_attn: float32 [1, 2048], P(None, ('dp', 'seq'))
- grad_gain_ffn: float32 [1, 2048], P(None, ('dp', 'seq'))
- grad_query: float32 [1, 2048, 2048], P(None, ('dp', 'seq'), 'tensor')
- grad_key: float32 [1, 2048, 512], P(None, ('dp', 'seq'), 'tensor')
- grad_value: float32 [1, 2048, 512], P(None, ('dp', 'seq'), 'tensor')
- grad_out: float32 [1, 2048, 2048], P(None, ('dp', 'seq'), 'tensor')
- grad_gate: float32 [1, 2048, 8192], P(None, ('dp', 'seq'), 'tensor')
- grad_up: float32 [1, 2048, 8192], P(None, ('dp', 'seq'), 'tensor')
- grad_down: float32 [1, 2048, 8192], P(None, ('dp', 'seq'), 'tensor')
The draws below stay inside these ranges and needn't reach their ends.
Inputs may be any that keep to these rules, and one draw needn't show every extreme that they name: In each sequence positions start at 0 and rise by 1 to 3 from one token to the next; the first sequence rises by 3 throughout.
All inputs are finite; a program needn't handle non-finite values.
Results may differ from the reference program's by a relative error of at most 0.018.
The reference program's roundings to bfloat16 on the way count: a program that leaves them out, or rounds other values in their place, can miss the bound.
Values may be sent and summed in bfloat16 or wider, within the bound.
A program may use at most 320 MiB of HBM per device.

```python
import jax
import jax.numpy as jnp
from jax import lax

D = 2048
HQ = 32
KV = 8
HD = 64
FF = 8192
LAYERS = 1
SEQS = 4
LEN = 512


plant_scale = 0.25


strength_levels = (1.0, 0.8, 0.6)


def draw_positions(key, part):
    steps_drawn = jax.random.randint(key, (SEQS, LEN), 1, 4)
    first_row = jnp.arange(SEQS, dtype=jnp.int32)[:, None] == 0
    steps_drawn = jnp.where(first_row, 3, steps_drawn)
    steps_drawn = jnp.where(jnp.arange(LEN, dtype=jnp.int32)[None, :] == 0, 0, steps_drawn)
    return jnp.cumsum(steps_drawn, axis=1).astype(jnp.int32)


def drawn_signs(key):
    feature_sign = (jax.random.randint(jax.random.fold_in(key, 11), (D,), 0, 2) * 2 - 1).astype(jnp.float32)
    head_sign = (jax.random.randint(jax.random.fold_in(key, 12), (HD,), 0, 2) * 2 - 1).astype(jnp.float32)
    return (feature_sign * D ** (-0.5), head_sign)


def draw_projection(key, salt_value, columns):
    direction, head_sign = drawn_signs(key)
    shape_full = (LAYERS, D, columns)
    base_part = jax.random.truncated_normal(jax.random.fold_in(key, salt_value), -6.0, 6.0, shape_full, jnp.float32)
    column_at = jnp.arange(columns, dtype=jnp.int32)
    planted = jnp.where(column_at < HD, head_sign[column_at % HD], 0.0)
    whole = base_part * D ** (-0.5) + plant_scale * direction[None, :, None] * planted[None, None, :]
    return whole.astype(jnp.bfloat16)


def draw_w_query(key, part):
    return draw_projection(key, 2, HQ * HD)


def draw_w_key(key, part):
    return draw_projection(key, 3, KV * HD)


def draw_tokens(key, part):
    direction, head_sign = drawn_signs(key)
    shape_full = (SEQS, LEN, D)
    jitter = jax.random.truncated_normal(jax.random.fold_in(key, 1), -6.0, 6.0, shape_full, jnp.float32)
    seq_at = jnp.arange(SEQS, dtype=jnp.int32)[:, None]
    row_at = jnp.arange(LEN, dtype=jnp.int32)[None, :]
    strength = jnp.zeros((SEQS, LEN), jnp.float32)
    for level_index in range(3):
        anchor = LEN - 1 - level_index * (LEN // 4)
        level_value = jnp.zeros((SEQS, 1), jnp.float32)
        for option_index in range(3):
            level_value = jnp.where((seq_at + level_index) % 3 == option_index, strength_levels[option_index], level_value)
        strength = jnp.where(row_at == anchor, level_value, strength)
        strength = jnp.where(row_at == anchor - 1, 0.95 * level_value, strength)
    remainder = jnp.sqrt(1.0 - strength * strength)
    whole = strength[..., None] * D ** 0.5 * direction[None, None, :] + remainder[..., None] * jitter
    return whole.astype(jnp.bfloat16)


def levels(rng, extent, cuts, smallest, top_value):
    def one(dim, shards_of):
        draws = jax.random.uniform(jax.random.fold_in(jax.random.fold_in(rng, 6), dim), (shards_of,), jnp.float32, smallest / len(cuts), top_value / len(cuts))
        return jnp.repeat(jnp.exp(draws), extent[dim] // shards_of).reshape((-1,) + (1,) * (len(extent) - dim - 1))

    factor_of = one(*cuts[0])
    for cut in cuts[1:]:
        factor_of = factor_of * one(*cut)
    return factor_of


def bell_draw(own_key, shape, spread, reach, split=(), kind=jnp.bfloat16):
    entries = spread * jax.random.normal(own_key, shape, jnp.float32)
    if split:
        entries = entries * levels(own_key, shape, split, -0.22, 0.18)
    return jnp.clip(entries, -reach, reach).astype(kind)


def setup_inputs(seed: int = 0) -> dict:
    keys = jax.random.split(jax.random.key(seed), 13)
    tokens = draw_tokens(jax.random.fold_in(keys[12], 71), 0)
    positions = draw_positions(jax.random.fold_in(keys[12], 71), 0)
    gain_attn = jnp.clip(1.0 + 0.1 * jax.random.normal(keys[2], (LAYERS, D), jnp.float32), 0.5, 1.5).astype(jnp.bfloat16)
    gain_ffn = jnp.clip(1.0 + 0.1 * jax.random.normal(keys[3], (LAYERS, D), jnp.float32), 0.5, 1.5).astype(jnp.bfloat16)
    w_query = draw_w_query(jax.random.fold_in(keys[12], 71), 0)
    w_key = draw_w_key(jax.random.fold_in(keys[12], 71), 0)
    w_value = bell_draw(keys[6], (LAYERS, D, KV * HD), D ** -0.5, 0.125, ((1, 16), (2, 2)))
    w_out = bell_draw(keys[7], (LAYERS, D, HQ * HD), HD ** -0.5, 0.75, ((1, 16), (2, 2)))
    w_gate = bell_draw(keys[8], (LAYERS, D, FF), D ** -0.5, 0.125, ((1, 16), (2, 2)))
    w_up = bell_draw(keys[9], (LAYERS, D, FF), D ** -0.5, 0.125, ((1, 16), (2, 2)))
    w_down = bell_draw(keys[10], (LAYERS, D, FF), FF ** -0.5, 0.0625, ((1, 16), (2, 2)))
    cotangent = bell_draw(keys[11], (SEQS, LEN, D), 1.0, 6.0, ((0, 4), (1, 4)))
    return dict(tokens=tokens, positions=positions, gain_attn=gain_attn, gain_ffn=gain_ffn, w_query=w_query, w_key=w_key, w_value=w_value, w_out=w_out, w_gate=w_gate, w_up=w_up, w_down=w_down, cotangent=cotangent)


epsilon = 1e-05
rope_base = 500000.0

def norm_forward(stream, gain):
    inverse = lax.rsqrt(lax.optimization_barrier(jnp.mean(stream * stream, axis=-1, keepdims=True)) + epsilon)
    return ((stream * inverse * gain.astype(jnp.float32)).astype(jnp.bfloat16), inverse)

def norm_backward(stream, inverse, gain, normed_grad):
    unit_rms = stream * inverse
    gain_grad = lax.optimization_barrier(jnp.sum(normed_grad * unit_rms, axis=0))
    scaled = normed_grad * gain.astype(jnp.float32)
    return (inverse * (scaled - unit_rms * lax.optimization_barrier(jnp.mean(scaled * unit_rms, axis=-1, keepdims=True))), gain_grad)

def rope_tables(position, head_dim):
    half_dim = head_dim // 2
    frequency = rope_base ** (-jnp.arange(half_dim, dtype=jnp.float32) / half_dim)
    angles = position.astype(jnp.float32)[:, None] * frequency[None, :]
    return (jnp.cos(angles)[:, None, :], jnp.sin(angles)[:, None, :])

def rotate(values, cosine, sine_table, direction):
    half_dim = values.shape[-1] // 2
    first_half = values[..., :half_dim]
    second_half = values[..., half_dim:]
    return jnp.concatenate([first_half * cosine - direction * second_half * sine_table, second_half * cosine + direction * first_half * sine_table], axis=-1)

def contract_last(left_matrix, right_matrix):
    return lax.dot_general(left_matrix, right_matrix, (((1,), (1,)), ((), ())), preferred_element_type=jnp.float32)

def contract_rows(left_matrix, right_matrix):
    return lax.dot_general(left_matrix, right_matrix, (((0,), (0,)), ((), ())), preferred_element_type=jnp.float32)

def head_scores(query_head, key_head, q_index):
    score_scale = query_head.shape[-1] ** (-0.5)
    raw_scores = jnp.einsum('qgd,kd->gqk', query_head.astype(jnp.float32), key_head.astype(jnp.float32)) * score_scale
    allowed = q_index[:, None] >= jnp.arange(key_head.shape[0], dtype=jnp.int32)[None, :]
    return jnp.where(allowed[None], raw_scores, -1e+30)

def attend(queries, keys_all, values_all, q_index):

    def one_head(operands):
        query_head, key_head, value_head = operands
        scores = head_scores(query_head, key_head, q_index)
        row_peak = lax.optimization_barrier(jnp.max(scores, axis=-1, keepdims=True))
        exps = jnp.exp(scores - row_peak)
        totals = lax.optimization_barrier(jnp.sum(exps, axis=-1, keepdims=True))
        probability = (exps / totals).astype(jnp.bfloat16)
        attended = jnp.einsum('gqk,kd->qgd', probability.astype(jnp.float32), value_head.astype(jnp.float32))
        return (attended.astype(jnp.bfloat16), (row_peak + jnp.log(totals))[..., 0])
    attended, logsum = lax.map(one_head, (jnp.moveaxis(queries, 1, 0), jnp.moveaxis(keys_all, 1, 0), jnp.moveaxis(values_all, 1, 0)))
    return (jnp.moveaxis(attended, 0, 1), logsum)

def attend_back(queries, keys_all, values_all, attended, attended_grad, logsum, q_index):

    def one_head(operands):
        query_head, key_head, value_head, mixed_head, grad_head, logsum_head = operands
        score_scale = query_head.shape[-1] ** (-0.5)
        probability = jnp.exp(head_scores(query_head, key_head, q_index) - logsum_head[..., None])
        value_grad = jnp.einsum('gqk,qgd->kd', probability.astype(jnp.bfloat16).astype(jnp.float32), grad_head.astype(jnp.float32))
        prob_grad = jnp.einsum('qgd,kd->gqk', grad_head.astype(jnp.float32), value_head.astype(jnp.float32))
        row_dots = lax.optimization_barrier(jnp.sum(grad_head.astype(jnp.float32) * mixed_head.astype(jnp.float32), axis=-1))
        score_grad = (probability * (prob_grad - row_dots.T[:, :, None]) * score_scale).astype(jnp.bfloat16)
        query_grad = jnp.einsum('gqk,kd->qgd', score_grad.astype(jnp.float32), key_head.astype(jnp.float32))
        key_grad = jnp.einsum('gqk,qgd->kd', score_grad.astype(jnp.float32), query_head.astype(jnp.float32))
        return (query_grad, key_grad, value_grad)
    query_grad, key_grad, value_grad = lax.map(one_head, (jnp.moveaxis(queries, 1, 0), jnp.moveaxis(keys_all, 1, 0), jnp.moveaxis(values_all, 1, 0), jnp.moveaxis(attended, 1, 0), jnp.moveaxis(attended_grad, 1, 0), logsum))
    return (jnp.moveaxis(query_grad, 0, 1), jnp.moveaxis(key_grad, 0, 1), jnp.moveaxis(value_grad, 0, 1))

def layer_forward(stream, cosine, sine_table, weights):
    gain_one, gain_two, w_q, w_k, w_v, w_o, w_g, w_u, w_d = weights
    row_count = stream.shape[0]
    q_index = jnp.arange(row_count, dtype=jnp.int32)
    normed_one, inverse_one = norm_forward(stream, gain_one)
    queries = rotate(jnp.dot(normed_one, w_q, preferred_element_type=jnp.float32).reshape(row_count, HQ, HD), cosine, sine_table, 1.0).astype(jnp.bfloat16)
    keys_all = rotate(jnp.dot(normed_one, w_k, preferred_element_type=jnp.float32).reshape(row_count, KV, HD), cosine, sine_table, 1.0).astype(jnp.bfloat16)
    values_all = jnp.dot(normed_one, w_v, preferred_element_type=jnp.float32).astype(jnp.bfloat16).reshape(row_count, KV, HD)
    attended, logsum = attend(queries.reshape(row_count, KV, HQ // KV, HD), keys_all, values_all, q_index)
    attended = attended.reshape(row_count, HQ * HD)
    after_attn = stream + contract_last(attended, w_o)
    normed_two, inverse_two = norm_forward(after_attn, gain_two)
    gate_pre = jnp.dot(normed_two, w_g, preferred_element_type=jnp.float32)
    up_proj = jnp.dot(normed_two, w_u, preferred_element_type=jnp.float32)
    hidden = (jax.nn.silu(gate_pre) * up_proj).astype(jnp.bfloat16)
    output = after_attn + contract_last(hidden, w_d)
    kept_state = (stream, inverse_one, normed_one, queries, keys_all, values_all, attended, logsum, after_attn, inverse_two, normed_two, gate_pre, up_proj, hidden)
    return (output, kept_state)

def layer_backward(out_grad, kept_state, cosine, sine_table, weights):
    gain_one, gain_two, w_q, w_k, w_v, w_o, w_g, w_u, w_d = weights
    stream, inverse_one, normed_one, queries, keys_all, values_all, attended, logsum, after_attn, inverse_two, normed_two, gate_pre, up_proj, hidden = kept_state
    row_count = stream.shape[0]
    q_index = jnp.arange(row_count, dtype=jnp.int32)
    low_grad = out_grad.astype(jnp.bfloat16)
    down_grad = contract_rows(low_grad, hidden)
    hidden_grad = jnp.dot(low_grad, w_d, preferred_element_type=jnp.float32)
    sigmoid_gate = jax.nn.sigmoid(gate_pre)
    gate_grad = (hidden_grad * up_proj * sigmoid_gate * (1.0 + gate_pre * (1.0 - sigmoid_gate))).astype(jnp.bfloat16)
    up_grad = (hidden_grad * gate_pre * sigmoid_gate).astype(jnp.bfloat16)
    wgate_grad = contract_rows(normed_two, gate_grad)
    wup_grad = contract_rows(normed_two, up_grad)
    normed_two_grad = contract_last(gate_grad, w_g) + contract_last(up_grad, w_u)
    resid_part, gain_two_grad = norm_backward(after_attn, inverse_two, gain_two, normed_two_grad)
    resid_grad = out_grad + resid_part
    resid_low = resid_grad.astype(jnp.bfloat16)
    wout_grad = contract_rows(resid_low, attended)
    attended_grad = jnp.dot(resid_low, w_o, preferred_element_type=jnp.float32).astype(jnp.bfloat16)
    group_shape = (row_count, KV, HQ // KV, HD)
    query_grad, key_grad, value_grad = attend_back(queries.reshape(group_shape), keys_all, values_all, attended.reshape(group_shape), attended_grad.reshape(group_shape), logsum, q_index)
    query_grad = rotate(query_grad.reshape(row_count, HQ, HD), cosine, sine_table, -1.0).astype(jnp.bfloat16).reshape(row_count, HQ * HD)
    key_grad = rotate(key_grad, cosine, sine_table, -1.0).astype(jnp.bfloat16).reshape(row_count, KV * HD)
    value_grad = value_grad.astype(jnp.bfloat16).reshape(row_count, KV * HD)
    wq_grad = contract_rows(normed_one, query_grad)
    wk_grad = contract_rows(normed_one, key_grad)
    wv_grad = contract_rows(normed_one, value_grad)
    normed_one_grad = contract_last(query_grad, w_q) + contract_last(key_grad, w_k) + contract_last(value_grad, w_v)
    input_part, gain_one_grad = norm_backward(stream, inverse_one, gain_one, normed_one_grad)
    return (resid_grad + input_part, (gain_one_grad, gain_two_grad, wq_grad, wk_grad, wv_grad, wout_grad, wgate_grad, wup_grad, down_grad))

def reference(tokens, positions, gain_attn, gain_ffn, w_query, w_key, w_value, w_out, w_gate, w_up, w_down, cotangent):
    shards = (gain_attn, gain_ffn, w_query, w_key, w_value, w_out, w_gate, w_up, w_down)

    def one_sequence(running, inputs):
        sequence, position, seq_cotangent = inputs
        cosine, sine_table = rope_tables(position, HD)
        stream = sequence.astype(jnp.float32)
        states = []
        for layer_at in range(LAYERS):
            stream, kept_state = layer_forward(stream, cosine, sine_table, tuple((member[layer_at] for member in shards)))
            states.append(kept_state)
        carried = seq_cotangent.astype(jnp.float32)
        layer_grads = [None] * LAYERS
        for layer_at in reversed(range(LAYERS)):
            carried, layer_grads[layer_at] = layer_backward(carried, states[layer_at], cosine, sine_table, tuple((member[layer_at] for member in shards)))
        updated = tuple((running[member] + jnp.stack([layer_grads[layer_at][member] for layer_at in range(LAYERS)]) for member in range(9)))
        return (updated, (stream.astype(jnp.bfloat16), carried))
    zeros_init = tuple((jnp.zeros(member.shape, jnp.float32) for member in shards))
    totals, (activations, input_grad) = lax.scan(one_sequence, zeros_init, (tokens, positions, cotangent))
    return (activations, input_grad, totals[0], totals[1], totals[2], totals[3], totals[4], totals[5], totals[6], totals[7], totals[8])
```

```python
import functools

import jax
import jax.numpy as jnp
from jax import lax
from jax.experimental import pallas as pl
from jax.experimental.pallas import tpu as pltpu
from jax.sharding import PartitionSpec as P

HD = 64
MESH = pl.DeviceIdType.MESH

epsilon = 1e-05
rope_base = 500000.0


class Net:
    def __init__(self, send_sems, recv_sems):
        self.send_sems, self.recv_sems = send_sems, recv_sems
        self.copies = []

    def send(self, source, target, device):
        at = len(self.copies)
        copy = pltpu.make_async_remote_copy(
            src_ref=source,
            dst_ref=target,
            send_sem=self.send_sems.at[at],
            recv_sem=self.recv_sems.at[at],
            device_id=device,
            device_id_type=MESH,
        )
        copy.start()
        self.copies.append(copy)
        return copy

    def drain(self):
        for copy in self.copies:
            copy.wait_send()


def greet(devices):
    barrier = pltpu.get_barrier_semaphore()
    for device in devices:
        pl.semaphore_signal(barrier, inc=1, device_id=device, device_id_type=MESH)
    pl.semaphore_wait(barrier, len(devices))


def shifted(at, offset, size):
    return lax.rem(at + offset, size)


def call_kernel(body, inputs, outputs, in_vmem, copies, local, ident, name, scratch=()):
    spaces = [
        pl.BlockSpec(memory_space=pltpu.VMEM if inside else pl.ANY) for inside in in_vmem
    ]
    return pl.pallas_call(
        body,
        out_shape=outputs,
        in_specs=spaces,
        out_specs=[pl.BlockSpec(memory_space=pl.ANY)] * len(outputs),
        scratch_shapes=[
            pltpu.SemaphoreType.DMA((max(copies, 1),)),
            pltpu.SemaphoreType.DMA((max(copies, 1),)),
            pltpu.SemaphoreType.DMA((max(local, 1),)),
            *scratch,
        ],
        compiler_params=pltpu.CompilerParams(collective_id=ident, has_side_effects=True),
        name=name,
    )(*inputs)


def intake_kernel(sizes, pack_a, pack_f, piece, notes, all_a, all_f, pieces, all_notes, ssem, rsem, lsem):
    dp, seq, _ = sizes
    z, s = lax.axis_index("dp"), lax.axis_index("seq")
    mine = z * seq + s
    offsets = [(oz, os) for oz in range(dp) for os in range(seq) if oz or os]
    where = {o: (shifted(z, o[0], dp), shifted(s, o[1], seq)) for o in offsets}
    ids = {o: {"dp": where[o][0], "seq": where[o][1]} for o in offsets}
    greet([ids[o] for o in offsets])
    net = Net(ssem, rsem)
    for o in offsets:
        net.send(notes, all_notes.at[mine], ids[o])
    for o in offsets:
        net.send(pack_a.at[where[o][1]], all_a.at[mine], ids[o])
        if not o[0]:
            net.send(piece, pieces.at[s], ids[o])
    for o in offsets:
        net.send(pack_f.at[where[o][0] * seq + where[o][1]], all_f.at[mine], ids[o])
    own = [
        pltpu.make_async_copy(notes, all_notes.at[mine], lsem.at[0]),
        pltpu.make_async_copy(pack_a.at[s], all_a.at[mine], lsem.at[1]),
        pltpu.make_async_copy(piece, pieces.at[s], lsem.at[2]),
        pltpu.make_async_copy(pack_f.at[mine], all_f.at[mine], lsem.at[3]),
    ]
    for copy in own:
        copy.start()
    for copy in own:
        copy.wait()
    for copy in net.copies:
        copy.wait_recv()
    net.drain()


def intake(sizes, pack_a, pack_f, piece, notes, ident):
    dp, seq, _ = sizes
    n = dp * seq
    like = lambda lead, a: jax.ShapeDtypeStruct((lead,) + a.shape, a.dtype)
    return call_kernel(
        functools.partial(intake_kernel, sizes),
        (pack_a, pack_f, piece, notes),
        [
            jax.ShapeDtypeStruct((n,) + pack_a.shape[1:], pack_a.dtype),
            jax.ShapeDtypeStruct(pack_f.shape, pack_f.dtype),
            like(seq, piece),
            like(n, notes),
        ],
        [True] * 4,
        3 * (n - 1) + seq - 1,
        4,
        ident,
        "intake",
    )


def plane_sum_kernel(sizes, parts, landed, ssem, rsem, lsem):
    _, seq, ten = sizes
    s, t = lax.axis_index("seq"), lax.axis_index("tensor")
    offsets = [(os, ot) for os in range(seq) for ot in range(ten) if os or ot]
    where = {o: (shifted(s, o[0], seq), shifted(t, o[1], ten)) for o in offsets}
    ids = {o: {"seq": where[o][0], "tensor": where[o][1]} for o in offsets}
    greet([ids[o] for o in offsets])
    net = Net(ssem, rsem)
    for at, o in enumerate(offsets):
        net.send(parts.at[where[o][0], where[o][1]], landed.at[at], ids[o])
    for copy in net.copies:
        copy.wait_recv()
    net.drain()


def plane_sum(sizes, partial_rows, ident):
    _, seq, ten = sizes
    rows = partial_rows.shape[0] // (seq * ten)
    parts = partial_rows.reshape(seq, ten, rows, -1)
    (landed,) = call_kernel(
        functools.partial(plane_sum_kernel, sizes),
        (parts,),
        [jax.ShapeDtypeStruct((seq * ten - 1,) + parts.shape[2:], parts.dtype)],
        [False],
        seq * ten - 1,
        0,
        ident,
        "plane_sum",
    )
    own = parts[lax.axis_index("seq"), lax.axis_index("tensor")]
    return own.astype(jnp.float32) + jnp.sum(landed.astype(jnp.float32), axis=0)


def plane_gather_kernel(sizes, rows, whole, ssem, rsem, lsem):
    _, seq, ten = sizes
    s, t = lax.axis_index("seq"), lax.axis_index("tensor")
    offsets = [(os, ot) for os in range(seq) for ot in range(ten) if os or ot]
    ids = {
        o: {"seq": shifted(s, o[0], seq), "tensor": shifted(t, o[1], ten)} for o in offsets
    }
    greet([ids[o] for o in offsets])
    net = Net(ssem, rsem)
    for o in offsets:
        net.send(rows, whole.at[s, t], ids[o])
    own = pltpu.make_async_copy(rows, whole.at[s, t], lsem.at[0])
    own.start()
    own.wait()
    for copy in net.copies:
        copy.wait_recv()
    net.drain()


def plane_gather(sizes, rows, ident):
    _, seq, ten = sizes
    (whole,) = call_kernel(
        functools.partial(plane_gather_kernel, sizes),
        (rows,),
        [jax.ShapeDtypeStruct((seq, ten) + rows.shape, rows.dtype)],
        [True],
        seq * ten - 1,
        1,
        ident,
        "plane_gather",
    )
    return whole.reshape(-1, rows.shape[-1])


def full_gather_kernel(sizes, rows, whole, ssem, rsem, lsem):
    dp, seq, ten = sizes
    inner = whole.shape[2]
    outer = seq // inner
    z, s, t = lax.axis_index("dp"), lax.axis_index("seq"), lax.axis_index("tensor")
    y, c = lax.div(s, inner), lax.rem(s, inner)
    half = rows.shape[-1] // 2
    front, back = pl.ds(0, half), pl.ds(half, half)
    to_dp = [{"dp": shifted(z, o, dp)} for o in range(1, dp)]
    to_ten = [{"tensor": shifted(t, o, ten)} for o in range(1, ten)]
    to_outer = [{"seq": shifted(y, o, outer) * inner + c} for o in range(1, outer)]
    to_inner = [{"seq": y * inner + shifted(c, o, inner)} for o in range(1, inner)]
    greet(to_dp + to_ten + to_outer + to_inner)
    net = Net(ssem, rsem)
    own = pltpu.make_async_copy(rows, whole.at[z, y, c, t], lsem.at[0])
    own.start()
    first = [net.send(rows, whole.at[z, y, c, t], device) for device in to_dp]
    came = [shifted(z, dp - k, dp) for k in range(dp)]
    second, third, fourth = {}, {}, {}
    for step in range(dp + 3):
        if step < dp:
            k = step
            if k:
                first[k - 1].wait_recv()
            block = rows if k == 0 else whole.at[came[k], y, c, t]
            there = whole.at[came[k], y, c, t]
            second[k] = [
                net.send(block.at[:, front], there.at[:, front], device) for device in to_ten
            ] + [net.send(block.at[:, back], there.at[:, back], device) for device in to_outer]
        if step == 0:
            own.wait()
        if 0 <= step - 1 < dp:
            k = step - 1
            for copy in second[k]:
                copy.wait_recv()
            strip = whole.at[came[k], y, c, :, :, front]
            stack = whole.at[came[k], :, c, t, :, back]
            third[k] = [net.send(strip, strip, device) for device in to_outer] + [
                net.send(stack, stack, device) for device in to_ten
            ]
        if 0 <= step - 2 < dp:
            k = step - 2
            for copy in third[k]:
                copy.wait_recv()
            side = whole.at[came[k], :, c]
            fourth[k] = [net.send(side, side, device) for device in to_inner]
        if 0 <= step - 3 < dp:
            for copy in fourth[step - 3]:
                copy.wait_recv()
    net.drain()


def full_gather(sizes, rows, ident):
    dp, seq, ten = sizes
    inner = 2 if seq % 2 == 0 else 1
    outer = seq // inner
    copies = dp - 1 + dp * (2 * (ten - 1) + 2 * (outer - 1) + inner - 1)
    (whole,) = call_kernel(
        functools.partial(full_gather_kernel, sizes),
        (rows,),
        [jax.ShapeDtypeStruct((dp, outer, inner, ten) + rows.shape, rows.dtype)],
        [True],
        copies,
        1,
        ident,
        "full_gather",
    )
    return whole.reshape(-1, rows.shape[-1])


def outtake_kernel(
    sizes, grad_a, grad_f, gains, row_grad, row_out, all_a, all_f, all_gains, pair_grad, pair_out,
    ssem, rsem, lsem,
):
    dp, seq, ten = sizes
    z, s, t = lax.axis_index("dp"), lax.axis_index("seq"), lax.axis_index("tensor")
    mine = z * seq + s
    offsets = [
        (oz, os, ot)
        for oz in range(dp)
        for os in range(seq)
        for ot in range(ten)
        if oz or os or ot
    ]
    where = {
        o: (shifted(z, o[0], dp), shifted(s, o[1], seq), shifted(t, o[2], ten)) for o in offsets
    }
    ids = {o: {"dp": where[o][0], "seq": where[o][1], "tensor": where[o][2]} for o in offsets}
    greet([ids[o] for o in offsets])
    net = Net(ssem, rsem)
    for o in offsets:
        owner = where[o][0] * seq + where[o][1]
        net.send(gains.at[owner], all_gains.at[z, s, t], ids[o])
        if o[2] == 0:
            net.send(grad_a.at[owner], all_a.at[mine], ids[o])
            net.send(grad_f.at[owner], all_f.at[mine], ids[o])
        if o[0] == 0 and o[1] == 0:
            net.send(row_grad, pair_grad.at[t], ids[o])
            net.send(row_out, pair_out.at[t], ids[o])
    own = [
        pltpu.make_async_copy(grad_a.at[mine], all_a.at[mine], lsem.at[0]),
        pltpu.make_async_copy(grad_f.at[mine], all_f.at[mine], lsem.at[1]),
        pltpu.make_async_copy(gains.at[mine], all_gains.at[z, s, t], lsem.at[2]),
        pltpu.make_async_copy(row_grad, pair_grad.at[t], lsem.at[3]),
        pltpu.make_async_copy(row_out, pair_out.at[t], lsem.at[4]),
    ]
    for copy in own:
        copy.start()
    for copy in own:
        copy.wait()
    for copy in net.copies:
        copy.wait_recv()
    net.drain()


def outtake(sizes, grad_a, grad_f, gains, row_grad, row_out, ident):
    dp, seq, ten = sizes
    n = dp * seq
    return call_kernel(
        functools.partial(outtake_kernel, sizes),
        (grad_a, grad_f, gains, row_grad, row_out),
        [
            jax.ShapeDtypeStruct(grad_a.shape, grad_a.dtype),
            jax.ShapeDtypeStruct(grad_f.shape, grad_f.dtype),
            jax.ShapeDtypeStruct((dp, seq, ten) + gains.shape[1:], gains.dtype),
            jax.ShapeDtypeStruct((ten,) + row_grad.shape, row_grad.dtype),
            jax.ShapeDtypeStruct((ten,) + row_out.shape, row_out.dtype),
        ],
        [True] * 5,
        n * ten - 1 + 2 * (n - 1) + 2 * (ten - 1),
        5,
        ident,
        "outtake",
    )


def full_sum(partial_rows):
    return lax.psum_scatter(
        partial_rows, ("dp", "seq", "tensor"), scatter_dimension=0, tiled=True
    ).astype(jnp.float32)


def norm_forward(stream, gain):
    inverse = lax.rsqrt(jnp.mean(stream * stream, axis=-1, keepdims=True) + epsilon)
    return ((stream * inverse * gain).astype(jnp.bfloat16), inverse)


def norm_backward(stream, inverse, gain, normed_grad):
    unit_rms = stream * inverse
    gain_grad = jnp.sum(normed_grad * unit_rms, axis=0)
    scaled = normed_grad * gain
    return (
        inverse * (scaled - unit_rms * jnp.mean(scaled * unit_rms, axis=-1, keepdims=True)),
        gain_grad,
    )


def rope_tables(position, head_dim):
    half_dim = head_dim // 2
    frequency = rope_base ** (-jnp.arange(half_dim, dtype=jnp.float32) / half_dim)
    angles = position[:, None] * frequency[None, :]
    return (jnp.cos(angles)[:, None, :], jnp.sin(angles)[:, None, :])


def rotate(values, cosine, sine_table, direction):
    half_dim = values.shape[-1] // 2
    first_half = values[..., :half_dim]
    second_half = values[..., half_dim:]
    return jnp.concatenate(
        [
            first_half * cosine - direction * second_half * sine_table,
            second_half * cosine + direction * first_half * sine_table,
        ],
        axis=-1,
    )


def dot(left, right):
    return jnp.dot(left, right, preferred_element_type=jnp.float32)


def dot_last(left, right):
    return lax.dot_general(
        left, right, (((1,), (1,)), ((), ())), preferred_element_type=jnp.float32
    )


def dot_rows(left, right):
    return lax.dot_general(
        left, right, (((0,), (0,)), ((), ())), preferred_element_type=jnp.float32
    )


def product(spec, left, right):
    return jnp.einsum(spec, left, right, preferred_element_type=jnp.float32)


def shards(
    sizes,
    tokens,
    positions,
    gain_attn,
    gain_ffn,
    w_query,
    w_key,
    w_value,
    w_out,
    w_gate,
    w_up,
    w_down,
    cotangent,
):
    dp, seq, ten = sizes
    n = dp * seq
    bf = jnp.bfloat16
    piece, width = tokens.shape[1:]
    band = w_query.shape[1]
    rows = piece // ten
    length = piece * seq
    s, t = lax.axis_index("seq"), lax.axis_index("tensor")

    q_cols = w_query.shape[2] // seq
    kv_local = w_key.shape[2] // HD
    repeat = max(1, seq // kv_local)
    k_cols = w_key.shape[2] * repeat // seq
    heads, groups = q_cols // HD, k_cols // HD
    per_group = heads // groups
    f_cols = w_gate.shape[2] // n

    def by_seq(weight, cols):
        return jnp.moveaxis(weight.reshape(band, -1, cols), 1, 0)

    pack_a = jnp.concatenate(
        [
            by_seq(w_query[0], q_cols),
            jnp.repeat(by_seq(w_key[0], k_cols), repeat, axis=0),
            jnp.repeat(by_seq(w_value[0], k_cols), repeat, axis=0),
            by_seq(w_out[0], q_cols),
        ],
        axis=-1,
    )
    pack_f = jnp.concatenate([by_seq(w[0], f_cols) for w in (w_gate, w_up, w_down)], axis=-1)
    span = -(-max(piece, band) // 128) * 128

    def note(values):
        values = values.reshape(1, -1).astype(jnp.float32)
        return jnp.pad(values, ((0, 7), (0, span - values.shape[1])))

    notes = jnp.concatenate([note(gain_attn), note(gain_ffn), note(positions)], axis=0)
    all_cotangent = lax.all_gather(cotangent[0], ("dp", "seq"), axis=0, tiled=True)
    all_a, all_f, pieces, all_notes = intake(sizes, pack_a, pack_f, tokens[0], notes, 0)
    gain_one = all_notes[:, 0, :band].reshape(1, width)
    gain_two = all_notes[:, 8, :band].reshape(1, width)
    z = lax.axis_index("dp")
    position = lax.dynamic_slice_in_dim(all_notes[:, 16, :piece], z * seq, seq, 0).reshape(length)
    all_a = all_a.reshape(width, -1)
    all_f = all_f.reshape(width, -1)
    w_qkv, w_o = all_a[:, : q_cols + 2 * k_cols], all_a[:, q_cols + 2 * k_cols :]
    w_gu, w_d = all_f[:, : 2 * f_cols], all_f[:, 2 * f_cols :]

    def own_rows(whole_piece):
        return lax.dynamic_slice_in_dim(whole_piece, t * rows, rows, 0)

    cosine, sine = rope_tables(position, HD)
    stream = pieces.reshape(length, width).astype(jnp.float32)
    normed_one, _ = norm_forward(stream, gain_one)
    qkv = dot(normed_one, w_qkv)
    queries = rotate(qkv[:, :q_cols].reshape(length, heads, HD), cosine, sine, 1.0).astype(bf)
    keys = rotate(
        qkv[:, q_cols : q_cols + k_cols].reshape(length, groups, HD), cosine, sine, 1.0
    ).astype(bf)
    values = qkv[:, q_cols + k_cols :].reshape(length, groups, HD).astype(bf)
    queries = queries.reshape(length, groups, per_group, HD)
    scale = HD**-0.5
    scores = product("qngd,knd->ngqk", queries, keys) * scale
    index = jnp.arange(length, dtype=jnp.int32)
    scores = jnp.where(index[:, None] >= index[None, :], scores, -1e30)
    exps = jnp.exp(scores - jnp.max(scores, axis=-1, keepdims=True))
    probability = exps / jnp.sum(exps, axis=-1, keepdims=True)
    low_probability = probability.astype(bf)
    attended = product("ngqk,knd->qngd", low_probability, values).astype(bf)
    flat_attended = attended.reshape(length, q_cols)
    mixed = plane_sum(sizes, dot_last(flat_attended, w_o).astype(bf), 1)
    row_stream = own_rows(tokens[0]).astype(jnp.float32)
    after_attn = row_stream + mixed

    row_normed, inverse_two = norm_forward(after_attn, gain_two)
    normed_two = full_gather(sizes, row_normed, 2)
    gate_up = dot(normed_two, w_gu)
    gate, up = gate_up[:, :f_cols], gate_up[:, f_cols:]
    sigmoid_gate = jax.nn.sigmoid(gate)
    hidden = (gate * sigmoid_gate * up).astype(bf)
    hidden_grad = dot(all_cotangent, w_d)
    gate_grad = (hidden_grad * up * sigmoid_gate * (1.0 + gate * (1.0 - sigmoid_gate))).astype(bf)
    up_grad = (hidden_grad * gate * sigmoid_gate).astype(bf)
    gu_grad = jnp.concatenate([gate_grad, up_grad], axis=-1)
    normed_two_grad = full_sum(dot_last(gu_grad, w_gu).astype(bf))
    row_out = after_attn + full_sum(dot_last(hidden, w_d).astype(bf))
    grad_f = jnp.concatenate(
        [dot_rows(normed_two, gu_grad), dot_rows(all_cotangent, hidden)], axis=-1
    ).astype(bf)

    row_cotangent = own_rows(cotangent[0]).astype(jnp.float32)
    part, gain_two_grad = norm_backward(after_attn, inverse_two, gain_two, normed_two_grad)
    resid_grad = row_cotangent + part

    resid_low = plane_gather(sizes, resid_grad.astype(bf), 3)
    attended_grad = dot(resid_low, w_o).astype(bf).reshape(attended.shape)
    value_grad = product("ngqk,qngd->knd", low_probability, attended_grad)
    prob_grad = product("qngd,knd->ngqk", attended_grad, values)
    row_dots = jnp.sum(attended_grad.astype(jnp.float32) * attended.astype(jnp.float32), axis=-1)
    score_grad = (
        probability * (prob_grad - jnp.moveaxis(row_dots, 0, -1)[..., None]) * scale
    ).astype(bf)
    query_grad = product("ngqk,knd->qngd", score_grad, keys).reshape(length, heads, HD)
    key_grad = product("ngqk,qngd->knd", score_grad, queries)
    qkv_grad = jnp.concatenate(
        [
            rotate(query_grad, cosine, sine, -1.0).reshape(length, q_cols),
            rotate(key_grad, cosine, sine, -1.0).reshape(length, k_cols),
            value_grad.reshape(length, k_cols),
        ],
        axis=-1,
    ).astype(bf)
    grad_a = jnp.concatenate(
        [dot_rows(normed_one, qkv_grad), dot_rows(resid_low, flat_attended)], axis=-1
    ).astype(bf)
    normed_one_grad = plane_sum(sizes, dot_last(qkv_grad, w_qkv).astype(bf), 4)
    inverse_one = lax.rsqrt(jnp.mean(row_stream * row_stream, axis=-1, keepdims=True) + epsilon)
    part, gain_one_grad = norm_backward(row_stream, inverse_one, gain_one, normed_one_grad)
    row_grad = resid_grad + part

    gains = jnp.pad(jnp.stack([gain_one_grad, gain_two_grad]), ((0, 6), (0, 0)))
    gains = jnp.moveaxis(gains.reshape(8, n, band), 1, 0)
    got_a, got_f, got_gains, pair_grad, pair_out = outtake(
        sizes,
        grad_a.reshape(n, band, -1),
        grad_f.reshape(n, band, -1),
        gains,
        row_grad,
        row_out.astype(bf),
        5,
    )
    got_a = jnp.sum(got_a.reshape(dp, seq, band, -1).astype(jnp.float32), axis=0)
    got_f = got_f.astype(jnp.float32)
    got_gains = jnp.sum(got_gains, axis=(0, 1, 2))

    def spread(block):
        return jnp.moveaxis(block, 0, 1).reshape(1, band, -1)

    def shared(block):
        return spread(jnp.sum(block.reshape(seq // repeat, repeat, band, k_cols), axis=1))

    return (
        pair_out.reshape(1, piece, width),
        pair_grad.reshape(1, piece, width),
        got_gains[0:1],
        got_gains[1:2],
        spread(got_a[..., :q_cols]),
        shared(got_a[..., q_cols : q_cols + k_cols]),
        shared(got_a[..., q_cols + k_cols : q_cols + 2 * k_cols]),
        spread(got_a[..., q_cols + 2 * k_cols :]),
        spread(got_f[..., :f_cols]),
        spread(got_f[..., f_cols : 2 * f_cols]),
        spread(got_f[..., 2 * f_cols :]),
    )


def solution(mesh):
    weight = P(None, ("dp", "seq"), "tensor")
    gain = P(None, ("dp", "seq"))
    rows = P("dp", "seq", None)
    in_specs = (rows, P("dp", "seq"), gain, gain) + (weight,) * 7 + (rows,)
    out_specs = (rows, rows, gain, gain) + (weight,) * 7
    sizes = (mesh.shape["dp"], mesh.shape["seq"], mesh.shape["tensor"])
    return jax.shard_map(
        functools.partial(shards, sizes),
        mesh=mesh,
        in_specs=in_specs,
        out_specs=out_specs,
        check_vma=False,
    )
```

```python
import functools

import jax
import jax.numpy as jnp
from jax import lax
from jax.experimental import pallas as pl
from jax.experimental.pallas import tpu as pltpu
from jax.sharding import PartitionSpec as P


HD = 64
MESH = pl.DeviceIdType.MESH

epsilon = 1e-05
rope_base = 500000.0


class Net:
    def __init__(self, send_sems, recv_sems):
        self.send_sems, self.recv_sems = send_sems, recv_sems
        self.copies = []

    def send(self, source, target, device):
        at = len(self.copies)
        copy = pltpu.make_async_remote_copy(
            src_ref=source,
            dst_ref=target,
            send_sem=self.send_sems.at[at],
            recv_sem=self.recv_sems.at[at],
            device_id=device,
            device_id_type=MESH,
        )
        copy.start()
        self.copies.append(copy)
        return copy

    def drain(self):
        for copy in self.copies:
            copy.wait_send()


def greet(devices):
    barrier = pltpu.get_barrier_semaphore()
    for device in devices:
        pl.semaphore_signal(barrier, inc=1, device_id=device, device_id_type=MESH)
    pl.semaphore_wait(barrier, len(devices))


def shifted(at, offset, size):
    return lax.rem(at + offset, size)


def call_kernel(body, inputs, outputs, in_vmem, copies, local, ident, scratch=()):
    spaces = [
        pl.BlockSpec(memory_space=pltpu.VMEM if inside else pl.ANY) for inside in in_vmem
    ]
    return pl.pallas_call(
        body,
        out_shape=outputs,
        in_specs=spaces,
        out_specs=[pl.BlockSpec(memory_space=pl.ANY)] * len(outputs),
        scratch_shapes=[
            pltpu.SemaphoreType.DMA((max(copies, 1),)),
            pltpu.SemaphoreType.DMA((max(copies, 1),)),
            pltpu.SemaphoreType.DMA((max(local, 1),)),
            *scratch,
        ],
        compiler_params=pltpu.CompilerParams(collective_id=ident, has_side_effects=True),
        cost_estimate=pl.CostEstimate(
            flops=0, bytes_accessed=40 * sum(a.size * a.dtype.itemsize for a in inputs), transcendentals=0
        ),
    )(*inputs)


def intake_kernel(sizes, pack_a, pack_f, piece, notes, all_a, staged_f, pieces, all_notes, ssem, rsem, lsem):
    dp, seq, _ = sizes
    z, s = lax.axis_index("dp"), lax.axis_index("seq")
    mine = z * seq + s
    offsets = [(oz, os) for oz in range(dp) for os in range(seq) if oz or os]
    where = {o: (shifted(z, o[0], dp), shifted(s, o[1], seq)) for o in offsets}
    ids = {o: {"dp": where[o][0], "seq": where[o][1]} for o in offsets}
    greet([ids[o] for o in offsets])
    net = Net(ssem, rsem)
    for o in offsets:
        net.send(notes, all_notes.at[mine], ids[o])
    for o in offsets:
        net.send(pack_a.at[where[o][1]], all_a.at[mine], ids[o])
        if not o[0]:
            net.send(piece, pieces.at[s], ids[o])
    for o in offsets:
        if not o[0]:
            net.send(pack_f.at[:, where[o][1]], staged_f.at[:, s], ids[o])
    own = [
        pltpu.make_async_copy(notes, all_notes.at[mine], lsem.at[0]),
        pltpu.make_async_copy(pack_a.at[s], all_a.at[mine], lsem.at[1]),
        pltpu.make_async_copy(piece, pieces.at[s], lsem.at[2]),
        pltpu.make_async_copy(pack_f.at[:, s], staged_f.at[:, s], lsem.at[3]),
    ]
    for copy in own:
        copy.start()
    for copy in own:
        copy.wait()
    for copy in net.copies:
        copy.wait_recv()
    net.drain()


def intake(sizes, pack_a, pack_f, piece, notes, ident):
    dp, seq, _ = sizes
    n = dp * seq
    like = lambda lead, a: jax.ShapeDtypeStruct((lead,) + a.shape, a.dtype)
    return call_kernel(
        functools.partial(intake_kernel, sizes),
        (pack_a, pack_f, piece, notes),
        [
            jax.ShapeDtypeStruct((n,) + pack_a.shape[1:], pack_a.dtype),
            jax.ShapeDtypeStruct(pack_f.shape, pack_f.dtype),
            like(seq, piece),
            like(n, notes),
        ],
        [True] * 4,
        2 * (n - 1) + 2 * (seq - 1),
        4,
        ident,
    )


def plane_sum_kernel(sizes, parts, landed, ssem, rsem, lsem):
    _, seq, ten = sizes
    s, t = lax.axis_index("seq"), lax.axis_index("tensor")
    offsets = [(os, ot) for os in range(seq) for ot in range(ten) if os or ot]
    where = {o: (shifted(s, o[0], seq), shifted(t, o[1], ten)) for o in offsets}
    ids = {o: {"seq": where[o][0], "tensor": where[o][1]} for o in offsets}
    greet([ids[o] for o in offsets])
    net = Net(ssem, rsem)
    for at, o in enumerate(offsets):
        net.send(parts.at[where[o][0], where[o][1]], landed.at[at], ids[o])
    for copy in net.copies:
        copy.wait_recv()
    net.drain()


def plane_sum(sizes, partial_rows, ident):
    _, seq, ten = sizes
    rows = partial_rows.shape[0] // (seq * ten)
    parts = partial_rows.reshape(seq, ten, rows, -1)
    (landed,) = call_kernel(
        functools.partial(plane_sum_kernel, sizes),
        (parts,),
        [jax.ShapeDtypeStruct((seq * ten - 1,) + parts.shape[2:], parts.dtype)],
        [False],
        seq * ten - 1,
        0,
        ident,
    )
    own = parts[lax.axis_index("seq"), lax.axis_index("tensor")]
    return own.astype(jnp.float32) + jnp.sum(landed.astype(jnp.float32), axis=0)


def plane_gather_kernel(sizes, rows, whole, ssem, rsem, lsem):
    _, seq, ten = sizes
    s, t = lax.axis_index("seq"), lax.axis_index("tensor")
    offsets = [(os, ot) for os in range(seq) for ot in range(ten) if os or ot]
    ids = {
        o: {"seq": shifted(s, o[0], seq), "tensor": shifted(t, o[1], ten)} for o in offsets
    }
    greet([ids[o] for o in offsets])
    net = Net(ssem, rsem)
    for o in offsets:
        net.send(rows, whole.at[s, t], ids[o])
    own = pltpu.make_async_copy(rows, whole.at[s, t], lsem.at[0])
    own.start()
    own.wait()
    for copy in net.copies:
        copy.wait_recv()
    net.drain()


def plane_gather(sizes, rows, ident):
    _, seq, ten = sizes
    (whole,) = call_kernel(
        functools.partial(plane_gather_kernel, sizes),
        (rows,),
        [jax.ShapeDtypeStruct((seq, ten) + rows.shape, rows.dtype)],
        [True],
        seq * ten - 1,
        1,
        ident,
    )
    return whole.reshape(-1, rows.shape[-1])


def full_gather_kernel(sizes, rows, whole, ssem, rsem, lsem):
    dp, seq, ten = sizes
    inner = whole.shape[2]
    outer = seq // inner
    z, s, t = lax.axis_index("dp"), lax.axis_index("seq"), lax.axis_index("tensor")
    y, c = lax.div(s, inner), lax.rem(s, inner)
    half = rows.shape[-1] // 2
    front, back = pl.ds(0, half), pl.ds(half, half)
    to_dp = [{"dp": shifted(z, o, dp)} for o in range(1, dp)]
    to_ten = [{"tensor": shifted(t, o, ten)} for o in range(1, ten)]
    to_outer = [{"seq": shifted(y, o, outer) * inner + c} for o in range(1, outer)]
    to_inner = [{"seq": y * inner + shifted(c, o, inner)} for o in range(1, inner)]
    greet(to_dp + to_ten + to_outer + to_inner)
    net = Net(ssem, rsem)
    own = pltpu.make_async_copy(rows, whole.at[z, y, c, t], lsem.at[0])
    own.start()
    first = [net.send(rows, whole.at[z, y, c, t], device) for device in to_dp]
    came = [shifted(z, dp - k, dp) for k in range(dp)]
    second, third, fourth = {}, {}, {}
    for step in range(dp + 3):
        if step < dp:
            k = step
            if k:
                first[k - 1].wait_recv()
            block = rows if k == 0 else whole.at[came[k], y, c, t]
            there = whole.at[came[k], y, c, t]
            second[k] = [
                net.send(block.at[:, front], there.at[:, front], device) for device in to_ten
            ] + [net.send(block.at[:, back], there.at[:, back], device) for device in to_outer]
        if step == 0:
            own.wait()
        if 0 <= step - 1 < dp:
            k = step - 1
            for copy in second[k]:
                copy.wait_recv()
            strip = whole.at[came[k], y, c, :, :, front]
            stack = whole.at[came[k], :, c, t, :, back]
            third[k] = [net.send(strip, strip, device) for device in to_outer] + [
                net.send(stack, stack, device) for device in to_ten
            ]
        if 0 <= step - 2 < dp:
            k = step - 2
            for copy in third[k]:
                copy.wait_recv()
            side = whole.at[came[k], :, c]
            fourth[k] = [net.send(side, side, device) for device in to_inner]
        if 0 <= step - 3 < dp:
            for copy in fourth[step - 3]:
                copy.wait_recv()
    net.drain()


def full_gather(sizes, rows, ident):
    dp, seq, ten = sizes
    inner = 2 if seq % 2 == 0 else 1
    outer = seq // inner
    copies = dp - 1 + dp * (2 * (ten - 1) + 2 * (outer - 1) + inner - 1)
    (whole,) = call_kernel(
        functools.partial(full_gather_kernel, sizes),
        (rows,),
        [jax.ShapeDtypeStruct((dp, outer, inner, ten) + rows.shape, rows.dtype)],
        [True],
        copies,
        1,
        ident,
    )
    return whole.reshape(-1, rows.shape[-1])


def outtake_kernel(
    sizes, grad_a, grad_f, gains, row_grad, row_out, all_a, all_f, all_gains, pair_grad, pair_out,
    ssem, rsem, lsem,
):
    dp, seq, ten = sizes
    z, s, t = lax.axis_index("dp"), lax.axis_index("seq"), lax.axis_index("tensor")
    mine = z * seq + s
    offsets = [
        (oz, os, ot)
        for oz in range(dp)
        for os in range(seq)
        for ot in range(ten)
        if oz or os or ot
    ]
    where = {
        o: (shifted(z, o[0], dp), shifted(s, o[1], seq), shifted(t, o[2], ten)) for o in offsets
    }
    ids = {o: {"dp": where[o][0], "seq": where[o][1], "tensor": where[o][2]} for o in offsets}
    greet([ids[o] for o in offsets])
    net = Net(ssem, rsem)
    for o in offsets:
        owner = where[o][0] * seq + where[o][1]
        net.send(gains.at[owner], all_gains.at[z, s, t], ids[o])
        if o[2] == 0:
            net.send(grad_a.at[owner], all_a.at[mine], ids[o])
        if o[0] == 0 and o[2] == 0:
            net.send(grad_f.at[:, where[o][1]], all_f.at[:, s], ids[o])
        if o[0] == 0 and o[1] == 0:
            net.send(row_grad, pair_grad.at[t], ids[o])
            net.send(row_out, pair_out.at[t], ids[o])
    own = [
        pltpu.make_async_copy(grad_a.at[mine], all_a.at[mine], lsem.at[0]),
        pltpu.make_async_copy(grad_f.at[:, s], all_f.at[:, s], lsem.at[1]),
        pltpu.make_async_copy(gains.at[mine], all_gains.at[z, s, t], lsem.at[2]),
        pltpu.make_async_copy(row_grad, pair_grad.at[t], lsem.at[3]),
        pltpu.make_async_copy(row_out, pair_out.at[t], lsem.at[4]),
    ]
    for copy in own:
        copy.start()
    for copy in own:
        copy.wait()
    for copy in net.copies:
        copy.wait_recv()
    net.drain()


def outtake(sizes, grad_a, grad_f, gains, row_grad, row_out, ident):
    dp, seq, ten = sizes
    n = dp * seq
    return call_kernel(
        functools.partial(outtake_kernel, sizes),
        (grad_a, grad_f, gains, row_grad, row_out),
        [
            jax.ShapeDtypeStruct(grad_a.shape, grad_a.dtype),
            jax.ShapeDtypeStruct(grad_f.shape, grad_f.dtype),
            jax.ShapeDtypeStruct((dp, seq, ten) + gains.shape[1:], gains.dtype),
            jax.ShapeDtypeStruct((ten,) + row_grad.shape, row_grad.dtype),
            jax.ShapeDtypeStruct((ten,) + row_out.shape, row_out.dtype),
        ],
        [True] * 5,
        n * ten - 1 + n - 1 + seq - 1 + 2 * (ten - 1),
        5,
        ident,
    )


def add_rows(target, sources):
    step = 16

    def body(at, carry):
        rows = pl.ds(at * step, step)
        total = target[rows].astype(jnp.float32)
        for source in sources:
            total += source[rows].astype(jnp.float32)
        target[rows] = total.astype(target.dtype)
        return carry

    lax.fori_loop(0, target.shape[0] // step, body, 0)


def full_sum_kernel(
    sizes, parts, total, ssem, rsem, lsem, held, from_inner, front_one, back_one, front_two,
    back_two, from_dp, result,
):
    dp, seq, ten = sizes
    inner = parts.shape[2]
    outer = seq // inner
    z, s, t = lax.axis_index("dp"), lax.axis_index("seq"), lax.axis_index("tensor")
    y, c = lax.div(s, inner), lax.rem(s, inner)
    half = parts.shape[-1] // 2
    front, back = pl.ds(0, half), pl.ds(half, half)
    to_dp = [{"dp": shifted(z, o, dp)} for o in range(1, dp)]
    ten_at = [shifted(t, o, ten) for o in range(ten)]
    outer_at = [shifted(y, o, outer) for o in range(outer)]
    inner_at = [shifted(c, o, inner) for o in range(inner)]
    to_ten = [{"tensor": at} for at in ten_at]
    to_outer = [{"seq": at * inner + c} for at in outer_at]
    to_inner = [{"seq": y * inner + at} for at in inner_at]
    greet(to_dp + to_ten[1:] + to_outer[1:] + to_inner[1:])
    net = Net(ssem, rsem)
    order = list(range(1, dp)) + [0]
    goal = [shifted(z, k, dp) for k in range(dp)]
    first, second, third, fourth, own = {}, {}, {}, {}, {}
    for k in order:
        own[k] = pltpu.make_async_copy(parts.at[goal[k], :, c], held.at[k], lsem.at[k])
        own[k].start()
        first[k] = [
            net.send(parts.at[goal[k], :, inner_at[o]], from_inner.at[k, o - 1], to_inner[o])
            for o in range(1, inner)
        ]
    for step in range(dp + 3):
        if step < dp:
            k = order[step]
            own[k].wait()
            for copy in first[k]:
                copy.wait_recv()
            for a in range(outer):
                for b in range(ten):
                    add_rows(
                        held.at[k, a, b], [from_inner.at[k, o, a, b] for o in range(inner - 1)]
                    )
            second[k] = [
                net.send(
                    held.at[k, outer_at[o], :, :, front], front_one.at[k, o - 1], to_outer[o]
                )
                for o in range(1, outer)
            ] + [
                net.send(held.at[k, :, ten_at[o], :, back], back_one.at[k, o - 1], to_ten[o])
                for o in range(1, ten)
            ]
        if 0 <= step - 1 < dp:
            k = order[step - 1]
            for copy in second[k]:
                copy.wait_recv()
            for b in range(ten):
                add_rows(
                    held.at[k, y, b, :, front], [front_one.at[k, o, b] for o in range(outer - 1)]
                )
            for a in range(outer):
                add_rows(
                    held.at[k, a, t, :, back], [back_one.at[k, o, a] for o in range(ten - 1)]
                )
            third[k] = [
                net.send(held.at[k, y, ten_at[o], :, front], front_two.at[k, o - 1], to_ten[o])
                for o in range(1, ten)
            ] + [
                net.send(held.at[k, outer_at[o], t, :, back], back_two.at[k, o - 1], to_outer[o])
                for o in range(1, outer)
            ]
        if 0 <= step - 2 < dp:
            k = order[step - 2]
            for copy in third[k]:
                copy.wait_recv()
            add_rows(held.at[k, y, t, :, front], [front_two.at[k, o] for o in range(ten - 1)])
            add_rows(held.at[k, y, t, :, back], [back_two.at[k, o] for o in range(outer - 1)])
            if k:
                fourth[k] = net.send(held.at[k, y, t], from_dp.at[k - 1], to_dp[k - 1])
    result[...] = held[0, y, t].astype(jnp.float32)
    for k in range(1, dp):
        fourth[k].wait_recv()
        add_rows(result, [from_dp.at[k - 1]])
    out = pltpu.make_async_copy(result, total, lsem.at[dp])
    out.start()
    out.wait()
    net.drain()


def full_sum(sizes, partial_rows, ident):
    dp, seq, ten = sizes
    inner = 2 if seq % 2 == 0 else 1
    outer = seq // inner
    width = partial_rows.shape[1]
    rows = partial_rows.shape[0] // (dp * seq * ten)
    half, bf = width // 2, partial_rows.dtype
    parts = partial_rows.reshape(dp, outer, inner, ten, rows, width)
    some = lambda count: max(count, 1)
    (total,) = call_kernel(
        functools.partial(full_sum_kernel, sizes),
        (parts,),
        [jax.ShapeDtypeStruct((rows, width), jnp.float32)],
        [False],
        dp - 1 + dp * (2 * (ten - 1) + 2 * (outer - 1) + inner - 1),
        dp + 1,
        ident,
        [
            pltpu.VMEM((dp, outer, ten, rows, width), bf),
            pltpu.VMEM((dp, some(inner - 1), outer, ten, rows, width), bf),
            pltpu.VMEM((dp, some(outer - 1), ten, rows, half), bf),
            pltpu.VMEM((dp, some(ten - 1), outer, rows, half), bf),
            pltpu.VMEM((dp, some(ten - 1), rows, half), bf),
            pltpu.VMEM((dp, some(outer - 1), rows, half), bf),
            pltpu.VMEM((some(dp - 1), rows, width), bf),
            pltpu.VMEM((rows, width), jnp.float32),
        ],
    )
    return total


def across_planes(dp, blocks):
    z = lax.axis_index("dp")
    leave = [lax.dynamic_index_in_dim(blocks, shifted(z, o, dp), 0) for o in range(1, dp)]
    *leave, blocks = lax.optimization_barrier((*leave, blocks))
    came = []
    for o, block in enumerate(leave, 1):
        came.append(lax.ppermute(block, "dp", [(i, (i + o) % dp) for i in range(dp)]))
    *came, blocks = lax.optimization_barrier((*came, blocks))
    for o, block in enumerate(came, 1):
        blocks = lax.dynamic_update_slice_in_dim(blocks, block, shifted(z, dp - o, dp), 0)
    return blocks


def norm_forward(stream, gain):
    inverse = lax.rsqrt(jnp.mean(stream * stream, axis=-1, keepdims=True) + epsilon)
    return ((stream * inverse * gain).astype(jnp.bfloat16), inverse)


def norm_backward(stream, inverse, gain, normed_grad):
    unit_rms = stream * inverse
    gain_grad = jnp.sum(normed_grad * unit_rms, axis=0)
    scaled = normed_grad * gain
    return (
        inverse * (scaled - unit_rms * jnp.mean(scaled * unit_rms, axis=-1, keepdims=True)),
        gain_grad,
    )


def rope_tables(position, head_dim):
    half_dim = head_dim // 2
    frequency = rope_base ** (-jnp.arange(half_dim, dtype=jnp.float32) / half_dim)
    angles = position[:, None] * frequency[None, :]
    return (jnp.cos(angles)[:, None, :], jnp.sin(angles)[:, None, :])


def rotate(values, cosine, sine_table, direction):
    half_dim = values.shape[-1] // 2
    first_half = values[..., :half_dim]
    second_half = values[..., half_dim:]
    return jnp.concatenate(
        [
            first_half * cosine - direction * second_half * sine_table,
            second_half * cosine + direction * first_half * sine_table,
        ],
        axis=-1,
    )


def dot(left, right):
    return jnp.dot(left, right, preferred_element_type=jnp.float32)


def dot_last(left, right):
    return lax.dot_general(
        left, right, (((1,), (1,)), ((), ())), preferred_element_type=jnp.float32
    )


def dot_rows(left, right):
    return lax.dot_general(
        left, right, (((0,), (0,)), ((), ())), preferred_element_type=jnp.float32
    )


def product(spec, left, right):
    return jnp.einsum(spec, left, right, preferred_element_type=jnp.float32)


def layer(
    sizes,
    tokens,
    positions,
    gain_attn,
    gain_ffn,
    w_query,
    w_key,
    w_value,
    w_out,
    w_gate,
    w_up,
    w_down,
    cotangent,
):
    dp, seq, ten = sizes
    n = dp * seq
    bf = jnp.bfloat16
    piece, width = tokens.shape[1:]
    band = w_query.shape[1]
    rows = piece // ten
    length = piece * seq
    t = lax.axis_index("tensor")

    q_cols = w_query.shape[2] // seq
    kv_local = w_key.shape[2] // HD
    repeat = max(1, seq // kv_local)
    k_cols = w_key.shape[2] * repeat // seq
    heads, groups = q_cols // HD, k_cols // HD
    per_group = heads // groups
    f_cols = w_gate.shape[2] // n

    def by_seq(weight, cols):
        return jnp.moveaxis(weight.reshape(band, -1, cols), 1, 0)

    pack_a = jnp.concatenate(
        [
            by_seq(w_query[0], q_cols),
            jnp.repeat(by_seq(w_key[0], k_cols), repeat, axis=0),
            jnp.repeat(by_seq(w_value[0], k_cols), repeat, axis=0),
            by_seq(w_out[0], q_cols),
        ],
        axis=-1,
    )
    pack_f = jnp.concatenate([by_seq(w[0], f_cols) for w in (w_gate, w_up, w_down)], axis=-1)
    span = -(-max(piece, band) // 128) * 128

    def note(values):
        values = values.reshape(1, -1).astype(jnp.float32)
        return jnp.pad(values, ((0, 7), (0, span - values.shape[1])))

    notes = jnp.concatenate([note(gain_attn), note(gain_ffn), note(positions)], axis=0)
    all_a, staged_f, pieces, all_notes = intake(
        sizes, pack_a, pack_f.reshape(dp, seq, band, -1), tokens[0], notes, 0
    )
    all_f = across_planes(dp, staged_f.reshape(dp, seq * band, -1))
    ready, _ = lax.optimization_barrier((cotangent[0], all_notes))
    all_cotangent = lax.all_gather(ready, ("dp", "seq"), axis=0, tiled=True)
    gain_one = all_notes[:, 0, :band].reshape(1, width)
    gain_two = all_notes[:, 8, :band].reshape(1, width)
    z = lax.axis_index("dp")
    position = lax.dynamic_slice_in_dim(all_notes[:, 16, :piece], z * seq, seq, 0).reshape(length)
    all_a = all_a.reshape(width, -1)
    all_f = all_f.reshape(width, -1)
    w_qkv, w_o = all_a[:, : q_cols + 2 * k_cols], all_a[:, q_cols + 2 * k_cols :]
    w_gu, w_d = all_f[:, : 2 * f_cols], all_f[:, 2 * f_cols :]

    def own_rows(whole_piece):
        return lax.dynamic_slice_in_dim(whole_piece, t * rows, rows, 0)

    cosine, sine = rope_tables(position, HD)
    stream = pieces.reshape(length, width).astype(jnp.float32)
    normed_one, _ = norm_forward(stream, gain_one)
    qkv = dot(normed_one, w_qkv)
    queries = rotate(qkv[:, :q_cols].reshape(length, heads, HD), cosine, sine, 1.0).astype(bf)
    keys = rotate(
        qkv[:, q_cols : q_cols + k_cols].reshape(length, groups, HD), cosine, sine, 1.0
    ).astype(bf)
    values = qkv[:, q_cols + k_cols :].reshape(length, groups, HD).astype(bf)
    queries = queries.reshape(length, groups, per_group, HD)
    scale = HD**-0.5
    scores = product("qngd,knd->ngqk", queries, keys) * scale
    index = jnp.arange(length, dtype=jnp.int32)
    scores = jnp.where(index[:, None] >= index[None, :], scores, -1e30)
    exps = jnp.exp(scores - jnp.max(scores, axis=-1, keepdims=True))
    probability = exps / jnp.sum(exps, axis=-1, keepdims=True)
    low_probability = probability.astype(bf)
    attended = product("ngqk,knd->qngd", low_probability, values).astype(bf)
    flat_attended = attended.reshape(length, q_cols)
    mixed = plane_sum(sizes, dot_last(flat_attended, w_o).astype(bf), 1)
    row_stream = own_rows(tokens[0]).astype(jnp.float32)
    after_attn = row_stream + mixed

    row_normed, inverse_two = norm_forward(after_attn, gain_two)
    normed_two = full_gather(sizes, row_normed, 2)
    gate_up = dot(normed_two, w_gu)
    gate, up = gate_up[:, :f_cols], gate_up[:, f_cols:]
    sigmoid_gate = jax.nn.sigmoid(gate)
    hidden = (gate * sigmoid_gate * up).astype(bf)
    hidden_grad = dot(all_cotangent, w_d)
    gate_grad = (hidden_grad * up * sigmoid_gate * (1.0 + gate * (1.0 - sigmoid_gate))).astype(bf)
    up_grad = (hidden_grad * gate * sigmoid_gate).astype(bf)
    gu_grad = jnp.concatenate([gate_grad, up_grad], axis=-1)
    normed_two_grad = full_sum(sizes, dot_last(gu_grad, w_gu).astype(bf), 6)
    down = dot_last(hidden, w_d).astype(bf)
    down = lax.psum_scatter(down, ("dp", "seq", "tensor"), scatter_dimension=0, tiled=True)
    grad_f = jnp.concatenate(
        [dot_rows(normed_two, gu_grad), dot_rows(all_cotangent, hidden)], axis=-1
    ).astype(bf)
    grad_f = across_planes(dp, grad_f.reshape(dp, seq * band, -1))

    row_cotangent = own_rows(cotangent[0]).astype(jnp.float32)
    part, gain_two_grad = norm_backward(after_attn, inverse_two, gain_two, normed_two_grad)
    resid_grad = row_cotangent + part

    resid_low = plane_gather(sizes, resid_grad.astype(bf), 3)
    attended_grad = dot(resid_low, w_o).astype(bf).reshape(attended.shape)
    value_grad = product("ngqk,qngd->knd", low_probability, attended_grad)
    prob_grad = product("qngd,knd->ngqk", attended_grad, values)
    row_dots = jnp.sum(attended_grad.astype(jnp.float32) * attended.astype(jnp.float32), axis=-1)
    score_grad = (
        probability * (prob_grad - jnp.moveaxis(row_dots, 0, -1)[..., None]) * scale
    ).astype(bf)
    query_grad = product("ngqk,knd->qngd", score_grad, keys).reshape(length, heads, HD)
    key_grad = product("ngqk,qngd->knd", score_grad, queries)
    qkv_grad = jnp.concatenate(
        [
            rotate(query_grad, cosine, sine, -1.0).reshape(length, q_cols),
            rotate(key_grad, cosine, sine, -1.0).reshape(length, k_cols),
            value_grad.reshape(length, k_cols),
        ],
        axis=-1,
    ).astype(bf)
    grad_a = jnp.concatenate(
        [dot_rows(normed_one, qkv_grad), dot_rows(resid_low, flat_attended)], axis=-1
    ).astype(bf)
    normed_one_grad = plane_sum(sizes, dot_last(qkv_grad, w_qkv).astype(bf), 4)
    down, normed_one_grad = lax.optimization_barrier((down, normed_one_grad))
    row_out = after_attn + down.astype(jnp.float32)
    inverse_one = lax.rsqrt(jnp.mean(row_stream * row_stream, axis=-1, keepdims=True) + epsilon)
    part, gain_one_grad = norm_backward(row_stream, inverse_one, gain_one, normed_one_grad)
    row_grad = resid_grad + part

    gains = jnp.pad(jnp.stack([gain_one_grad, gain_two_grad]), ((0, 6), (0, 0)))
    gains = jnp.moveaxis(gains.reshape(8, n, band), 1, 0)
    got_a, got_f, got_gains, pair_grad, pair_out = outtake(
        sizes,
        grad_a.reshape(n, band, -1),
        grad_f.reshape(dp, seq, band, -1),
        gains,
        row_grad,
        row_out.astype(bf),
        5,
    )
    got_a = jnp.sum(got_a.reshape(dp, seq, band, -1).astype(jnp.float32), axis=0)
    got_f = got_f.reshape(n, band, -1).astype(jnp.float32)
    got_gains = jnp.sum(got_gains, axis=(0, 1, 2))

    def spread(block):
        return jnp.moveaxis(block, 0, 1).reshape(1, band, -1)

    def shared(block):
        return spread(jnp.sum(block.reshape(seq // repeat, repeat, band, k_cols), axis=1))

    return (
        pair_out.reshape(1, piece, width),
        pair_grad.reshape(1, piece, width),
        got_gains[0:1],
        got_gains[1:2],
        spread(got_a[..., :q_cols]),
        shared(got_a[..., q_cols : q_cols + k_cols]),
        shared(got_a[..., q_cols + k_cols : q_cols + 2 * k_cols]),
        spread(got_a[..., q_cols + 2 * k_cols :]),
        spread(got_f[..., :f_cols]),
        spread(got_f[..., f_cols : 2 * f_cols]),
        spread(got_f[..., 2 * f_cols :]),
    )


def solution(mesh):
    weight = P(None, ("dp", "seq"), "tensor")
    gain = P(None, ("dp", "seq"))
    rows = P("dp", "seq", None)
    in_specs = (rows, P("dp", "seq"), gain, gain) + (weight,) * 7 + (rows,)
    out_specs = (rows, rows, gain, gain) + (weight,) * 7
    sizes = (mesh.shape["dp"], mesh.shape["seq"], mesh.shape["tensor"])
    return jax.shard_map(
        functools.partial(layer, sizes),
        mesh=mesh,
        in_specs=in_specs,
        out_specs=out_specs,
        check_vma=False,
    )
```
